32 devices in a mesh: dp: 4 (over y, x), context: 4 (over z), head: 2 (over core).
Axes of the slice: x: 2, y: 2, z: 4, core: 2. Of those that a mesh axis runs over, the one named last changes fastest.
Arguments:
- tokens: bfloat16 [4, 2, 512, 4096], P('dp', None, 'context', 'head'), may hold values from -7 to 7
- queries: bfloat16 [4, 2, 512, 2048], P('dp', None, 'context', 'head'), may hold values from -160 to 160
- grad_out: bfloat16 [4, 2, 512, 2048], P('dp', None, 'context', 'head'), may hold values from -6 to 6
- w_key: bfloat16 [4096, 256], P('context', 'head'), may hold values from -0.09375 to 0.09375
- w_value: bfloat16 [4096, 256], P('context', 'head'), may hold values from -0.09375 to 0.09375
- block_len: int32 [4], P('dp'), may hold values from 8 to 32, as said below
Outputs:
- grad_query: bfloat16 [4, 2, 512, 2048], P('dp', None, 'context', 'head')
- grad_x: bfloat16 [4, 2, 512, 4096], P('dp', None, 'context', 'head')
- grad_wkey: float32 [4096, 256], P('context', 'head')
- grad_wvalue: float32 [4096, 256], P('context', 'head')
The draws below stay inside these ranges and needn't reach their ends.
Inputs may be any that keep to these rules, and one draw needn't show every extreme that they name: `block_len`: each entry is 8, 16 or 32.
All inputs are finite; a program needn't handle non-finite values.
Results may differ from the reference program's by a relative error of at most 0.025.
Values may be sent and summed in bfloat16 or wider, within the bound.
A program may use at most 64 MiB of HBM per device.

```python
import math
import jax
import jax.numpy as jnp
from jax import lax

D = 4096
HEADS = 16
KV_HEADS = 2
HEAD_DIM = 128
CL_DEV = 128
LC = 512
REPLICAS = 4
N_CONTEXT = 4


def shared_arrays(key):
    token_key, weight_key, query_key = jax.random.split(jax.random.fold_in(key, 11), 3)
    length = CL_DEV * N_CONTEXT
    tokens = jnp.clip(jax.random.normal(token_key, (REPLICAS, 2, length, D), jnp.float32), -6.0, 6.0)
    w_key = jnp.clip(jax.random.normal(weight_key, (D, KV_HEADS * HEAD_DIM), jnp.float32), -6.0, 6.0) / math.sqrt(D)
    queries = jnp.clip(jax.random.normal(query_key, (REPLICAS, 2, length, HEADS * HEAD_DIM), jnp.float32), -6.0, 6.0)
    return (tokens, w_key, queries)


def draw_tokens(key, part):
    return shared_arrays(key)[0].astype(jnp.bfloat16)


def draw_w_key(key, part):
    return shared_arrays(key)[1].astype(jnp.bfloat16)


def draw_queries(key, part):
    return shared_arrays(key)[2].astype(jnp.bfloat16)


def draw_block_len(key, part):
    order = jax.random.permutation(jax.random.fold_in(key, 7), jnp.arange(REPLICAS, dtype=jnp.int32))
    exponent = 3 + order % 3
    return jnp.left_shift(jnp.ones((REPLICAS,), jnp.int32), exponent.astype(jnp.int32))


def level_of(own_key, dims, shards, low, top_value):
    loudness, own = 1.0, jax.random.fold_in(own_key, 6)
    for axis_at, parts in shards:
        draws = jnp.exp(jax.random.uniform(jax.random.fold_in(own, axis_at), (parts,), jnp.float32, low / len(shards), top_value / len(shards)))
        loudness = loudness * jnp.repeat(draws, dims[axis_at] // parts).reshape([-1 if axis == axis_at else 1 for axis in range(len(dims))])
    return loudness


def normal_values(key, dims, deviation, bound, cuts=(), kind=jnp.bfloat16):
    result = jax.random.normal(key, dims, jnp.float32) * deviation
    if len(cuts) > 0:
        result = level_of(key, dims, cuts, -0.22, 0.18) * result
    return jnp.clip(result, min=-bound, max=bound).astype(kind)


def setup_inputs(seed: int = 0) -> dict:
    arg_keys = jax.random.split(jax.random.key(seed), 7)
    tokens = draw_tokens(jax.random.fold_in(arg_keys[6], 71), 0)
    queries = draw_queries(jax.random.fold_in(arg_keys[6], 71), 0)
    grad_out = normal_values(arg_keys[2], (REPLICAS, 2, LC, HEADS * HEAD_DIM), 1.0, 6.0, ((0, 4), (2, 4), (3, 2)))
    w_key = draw_w_key(jax.random.fold_in(arg_keys[6], 71), 0)
    w_value = normal_values(arg_keys[4], (D, KV_HEADS * HEAD_DIM), D ** -0.5, 0.09375, ((0, 4), (1, 2)))
    block_len = draw_block_len(jax.random.fold_in(arg_keys[6], 71), 0)
    return {"tokens": tokens, "queries": queries, "grad_out": grad_out, "w_key": w_key, "w_value": w_value, "block_len": block_len}


masked_score = -1e+30

def rounded(values):
    return lax.optimization_barrier(values.astype(jnp.bfloat16)).astype(jnp.float32)

def matmul(left, right):
    return jnp.dot(left, right, precision=lax.Precision.HIGHEST)

def tile_einsum(form, left, right):
    return jnp.einsum(form, left, right, precision=lax.Precision.HIGHEST)

def one_head(q_clean, q_noisy, g_clean, g_noisy, k_clean, v_clean, k_noisy, v_noisy, block_size):
    score_scale = 1.0 / math.sqrt(HEAD_DIM)
    length = CL_DEV * N_CONTEXT
    position = jnp.arange(length, dtype=jnp.int32) // block_size
    see_clean = position[None, :] <= position[:, None]
    see_cross = position[None, :] < position[:, None]
    local_block = jnp.arange(CL_DEV, dtype=jnp.int32) // block_size
    see_own = local_block[None, :] == local_block[:, None]
    tile_shape = (N_CONTEXT, CL_DEV, HEAD_DIM)
    qn_tiles = q_noisy.reshape(tile_shape)
    gn_tiles = g_noisy.reshape(tile_shape)
    kn_tiles = k_noisy.reshape(tile_shape)
    vn_tiles = v_noisy.reshape(tile_shape)
    s_cc = jnp.where(see_clean, matmul(q_clean, k_clean.T) * score_scale, masked_score)
    s_nc = jnp.where(see_cross, matmul(q_noisy, k_clean.T) * score_scale, masked_score)
    s_nn = jnp.where(see_own, tile_einsum('tqd,tkd->tqk', qn_tiles, kn_tiles) * score_scale, masked_score)
    peak_c = lax.optimization_barrier(jnp.max(s_cc, axis=1))
    lse_c = peak_c + jnp.log(lax.optimization_barrier(jnp.sum(jnp.exp(s_cc - peak_c[:, None]), axis=1)))
    peak_n = jnp.maximum(lax.optimization_barrier(jnp.max(s_nc, axis=1)), lax.optimization_barrier(jnp.max(s_nn, axis=2)).reshape(length))
    peak_tiles = peak_n.reshape(N_CONTEXT, CL_DEV)
    total_n = lax.optimization_barrier(jnp.sum(jnp.exp(s_nc - peak_n[:, None]), axis=1))
    total_n = total_n + lax.optimization_barrier(jnp.sum(jnp.exp(s_nn - peak_tiles[:, :, None]), axis=2)).reshape(length)
    lse_n = peak_n + jnp.log(total_n)
    p_cc = jnp.exp(s_cc - lse_c[:, None])
    p_nc = jnp.exp(s_nc - lse_n[:, None])
    p_nn = jnp.exp(s_nn - lse_n.reshape(N_CONTEXT, CL_DEV)[:, :, None])
    half_cc = rounded(p_cc)
    half_nc = rounded(p_nc)
    half_nn = rounded(p_nn)
    out_c = matmul(half_cc, v_clean)
    out_n = matmul(half_nc, v_clean) + tile_einsum('tqk,tkd->tqd', half_nn, vn_tiles).reshape(length, HEAD_DIM)
    delta_c = lax.optimization_barrier(jnp.sum(g_clean * out_c, axis=1))
    delta_n = lax.optimization_barrier(jnp.sum(g_noisy * out_n, axis=1))
    ds_cc = rounded(p_cc * (matmul(g_clean, v_clean.T) - delta_c[:, None]))
    ds_nc = rounded(p_nc * (matmul(g_noisy, v_clean.T) - delta_n[:, None]))
    dp_nn = tile_einsum('tqd,tkd->tqk', gn_tiles, vn_tiles)
    ds_nn = rounded(p_nn * (dp_nn - delta_n.reshape(N_CONTEXT, CL_DEV)[:, :, None]))
    dq_c = matmul(ds_cc, k_clean) * score_scale
    dq_n = (matmul(ds_nc, k_clean) + tile_einsum('tqk,tkd->tqd', ds_nn, kn_tiles).reshape(length, HEAD_DIM)) * score_scale
    dk_c = (matmul(ds_cc.T, q_clean) + matmul(ds_nc.T, q_noisy)) * score_scale
    dv_c = matmul(half_cc.T, g_clean) + matmul(half_nc.T, g_noisy)
    dk_n = tile_einsum('tqk,tqd->tkd', ds_nn, qn_tiles).reshape(length, HEAD_DIM) * score_scale
    dv_n = tile_einsum('tqk,tqd->tkd', half_nn, gn_tiles).reshape(length, HEAD_DIM)
    return (jnp.stack([dq_c, dq_n]), jnp.stack([dk_c, dk_n]), jnp.stack([dv_c, dv_n]))

def reference(tokens, queries, grad_out, w_key, w_value, block_len):
    length = CL_DEV * N_CONTEXT
    group_size = HEADS // KV_HEADS
    flat_tokens = tokens.reshape(-1, D)
    key_flat = jnp.dot(flat_tokens, w_key, preferred_element_type=jnp.float32).astype(jnp.bfloat16)
    value_flat = jnp.dot(flat_tokens, w_value, preferred_element_type=jnp.float32).astype(jnp.bfloat16)

    def by_head(array, head_count):
        shaped = array.astype(jnp.float32).reshape(REPLICAS, 2, length, head_count, HEAD_DIM)
        return shaped.transpose(0, 3, 1, 2, 4).reshape(REPLICAS * head_count, 2, length, HEAD_DIM)
    key_heads = by_head(key_flat, KV_HEADS)
    value_heads = by_head(value_flat, KV_HEADS)
    query_heads = by_head(queries, HEADS)
    grad_heads = by_head(grad_out, HEADS)
    items = jnp.arange(REPLICAS * HEADS, dtype=jnp.int32)

    def run_item(index):
        replica = index // HEADS
        kv_index = replica * KV_HEADS + index % HEADS // group_size
        q_head = query_heads[index]
        g_head = grad_heads[index]
        k_head = key_heads[kv_index]
        v_head = value_heads[kv_index]
        return one_head(q_head[0], q_head[1], g_head[0], g_head[1], k_head[0], v_head[0], k_head[1], v_head[1], block_len[replica])
    dq_items, dk_items, dv_items = lax.map(run_item, items)
    grad_query = dq_items.reshape(REPLICAS, HEADS, 2, length, HEAD_DIM).transpose(0, 2, 3, 1, 4)
    grad_query = grad_query.reshape(REPLICAS, 2, length, HEADS * HEAD_DIM).astype(jnp.bfloat16)

    def group_sum(items_grad):
        summed = items_grad.reshape(REPLICAS, KV_HEADS, group_size, 2, length, HEAD_DIM).sum(axis=2)
        summed = summed.transpose(0, 2, 3, 1, 4).reshape(REPLICAS * 2 * length, KV_HEADS * HEAD_DIM)
        return summed.astype(jnp.bfloat16)
    grad_key = group_sum(dk_items)
    grad_value = group_sum(dv_items)
    grad_x = jnp.dot(grad_key, w_key.T, preferred_element_type=jnp.float32)
    grad_x = grad_x + jnp.dot(grad_value, w_value.T, preferred_element_type=jnp.float32)
    grad_x = grad_x.astype(jnp.bfloat16).reshape(tokens.shape)
    grad_wkey = jnp.dot(flat_tokens.T, grad_key, preferred_element_type=jnp.float32)
    grad_wvalue = jnp.dot(flat_tokens.T, grad_value, preferred_element_type=jnp.float32)
    return (grad_query, grad_x, grad_wkey, grad_wvalue)
```

```python
import functools
import math

import jax
import jax.numpy as jnp
from jax import lax
from jax.experimental import pallas as pl
from jax.experimental.pallas import tpu as pltpu
from jax.sharding import PartitionSpec as P

HEAD_DIM = 128
MASKED = -1e30
MESH = pl.DeviceIdType.MESH
NT = (((1,), (1,)), ((), ()))


def near_first(count):
    order = []
    for step in range(1, count):
        for offset in (step, count - step):
            if offset not in order:
                order.append(offset)
    return order


def dot(left, right):
    return jnp.dot(left, right, preferred_element_type=jnp.float32)


def dot_nt(left, right):
    return lax.dot_general(left, right, NT, preferred_element_type=jnp.float32)


def fused_kernel(
    n, m, share, early,
    blk_ref, tok_ref, q_ref, g_ref, wk_ref, wv_ref,
    dq_ref, gx_ref, gw_ref,
    tokf, wf, wo, kv, kvn, kt, knt, dkv, dn, pgp, pin, pga, pgo, tokd, gsum, rp, rin, rall,
    loc_sem, tok_sem, wz_s, wz_r, wd_s, wd_r, wx_s, wx_r, wo_sem, kv_s, kv_r,
    td_s, td_r, tf_s, tf_r, pp_s, pp_r, pn_s, pn_r, pc_s, pc_r, po_sem, rs_s, rs_r, ra_s, ra_r,
):
    me_dp = lax.axis_index("dp")
    me = lax.axis_index("context")
    head = lax.axis_index("head")
    other = 1 - head
    rows2, features = tok_ref.shape
    rows = rows2 // 2
    wrows = wk_ref.shape[0]
    half = n // 2
    score_scale = 1.0 / math.sqrt(HEAD_DIM)
    sends = []

    def copy_of(src, dst, send_sem, recv_sem, **device):
        return pltpu.make_async_remote_copy(
            src_ref=src, dst_ref=dst, send_sem=send_sem, recv_sem=recv_sem,
            device_id=device, device_id_type=MESH,
        )

    def put(src, dst, send_sem, recv_sem, **device):
        copy = copy_of(src, dst, send_sem, recv_sem, **device)
        copy.start()
        sends.append(copy)

    def arrived(dst, send_sem, recv_sem):
        copy_of(dst, dst, send_sem, recv_sem, head=other).wait_recv()

    ctx_peers = [(off, lax.rem(me + off, n)) for off in near_first(n)]
    dp_peers = [(off, lax.rem(me_dp + off, m)) for off in near_first(m)]

    own_copies = [
        pltpu.make_async_copy(wk_ref, wf.at[me, :, pl.ds(0, HEAD_DIM)], loc_sem.at[0]),
        pltpu.make_async_copy(wv_ref, wf.at[me, :, pl.ds(HEAD_DIM, HEAD_DIM)], loc_sem.at[1]),
        pltpu.make_async_copy(tok_ref, tokf.at[head], loc_sem.at[2]),
    ]
    for copy in own_copies:
        copy.start()

    barrier = pltpu.get_barrier_semaphore()
    for _, peer in ctx_peers:
        pl.semaphore_signal(barrier, inc=1, device_id={"context": peer}, device_id_type=MESH)
    for _, peer in dp_peers:
        pl.semaphore_signal(barrier, inc=1, device_id={"dp": peer}, device_id_type=MESH)
    pl.semaphore_signal(barrier, inc=1, device_id={"head": other}, device_id_type=MESH)
    pl.semaphore_wait(barrier, n + m - 1)

    put(tok_ref, tokf.at[head], tok_sem.at[0], tok_sem.at[1], head=other)
    own_copies[0].wait()
    own_copies[1].wait()
    shared = pl.ds(pl.multiple_of(me_dp * share, 16), share)
    direct_rows = wrows - m * share
    direct = pl.ds(m * share, direct_rows)
    for off, peer in ctx_peers:
        part = wf.at[me, shared]
        put(part, part, wz_s.at[off], wz_r.at[me], context=peer)
    if direct_rows:
        for off, peer in ctx_peers:
            part = wf.at[me, direct]
            put(part, part, wd_s.at[off], wd_r.at[me], context=peer)
    own_copies[2].wait()
    arrived(tokf.at[other], tok_sem.at[0], tok_sem.at[1])

    def token_block(owner):
        column = pl.multiple_of(lax.rem(owner, half) * wrows, 128)
        return owner // half, pl.ds(column, wrows)

    def token_rows(core, part):
        start = 0 if part == 0 else early
        count = early if part == 0 else rows - early
        return pl.ds(pl.multiple_of(core * rows + start, 16), count)

    def send_tokens(part):
        span = token_rows(head, part)
        for off, peer in ctx_peers:
            side, columns = token_block(peer)
            put(
                tokf.at[side, span, columns], tokd.at[me, span],
                td_s.at[part, off], td_r.at[part, me], context=peer,
            )

    my_side, my_columns = token_block(me)
    own_tokens = pltpu.make_async_copy(tokf.at[my_side, :, my_columns], tokd.at[me], loc_sem.at[3])
    own_tokens.start()
    for off, src in ctx_peers:
        part = wf.at[src, shared]
        arrived(part, wz_s.at[off], wz_r.at[src])
        for dp_off, peer in dp_peers:
            put(part, part, wx_s.at[src, dp_off], wx_r.at[src, me_dp], dp=peer)
    send_tokens(0)

    projected = dot(tokf[my_side, :, my_columns], wf[me])
    for off, src in ctx_peers:
        if direct_rows:
            arrived(wf.at[src, direct], wd_s.at[off], wd_r.at[src])
        for dp_off, peer in dp_peers:
            theirs = pl.ds(pl.multiple_of(peer * share, 16), share)
            arrived(wf.at[src, theirs], wx_s.at[src, dp_off], wx_r.at[src, peer])
        side, columns = token_block(src)
        projected += dot(tokf[side, :, columns], wf[src])
    pairs = projected.astype(jnp.bfloat16)
    my_rows = pl.ds(pl.multiple_of(me * rows, rows), rows)
    kv[my_rows, :] = pairs[:rows]
    kvn[...] = pairs[rows:]
    for off, peer in ctx_peers:
        put(kv.at[my_rows], kv.at[my_rows], kv_s.at[off], kv_r.at[me], context=peer)
    put(wf.at[pl.ds(other * half, half)], wo, wo_sem.at[0], wo_sem.at[1], head=other)
    send_tokens(1)

    block = blk_ref[0]
    total_rows = n * rows
    lane = lax.broadcasted_iota(jnp.int32, (1, rows2), 1)
    noisy_lane = lane >= rows
    position = me * rows + jnp.where(noisy_lane, lane - rows, lane)
    block_start = position & (-block)
    limit = jnp.where(noisy_lane, block_start, block_start + block)
    dkv[...] = jnp.zeros_like(dkv)
    dn[...] = jnp.zeros_like(dn)
    knt[...] = kvn[:, :HEAD_DIM].T
    for off, src in ctx_peers:
        span = pl.ds(pl.multiple_of(src * rows, rows), rows)
        arrived(kv.at[span], kv_s.at[off], kv_r.at[src])
    kt[...] = kv[:, :HEAD_DIM].T

    def head_turn(turn, carry):
        columns = pl.ds(pl.multiple_of(turn * HEAD_DIM, HEAD_DIM), HEAD_DIM)
        q = q_ref[:, columns]
        g = g_ref[:, columns]
        keys = kv[:, :HEAD_DIM]
        values = kv[:, HEAD_DIM:]
        own_keys = kvn[:, :HEAD_DIM]
        own_values = kvn[:, HEAD_DIM:]
        key_pos = lax.broadcasted_iota(jnp.int32, (total_rows, rows2), 0)
        near = lax.broadcasted_iota(jnp.int32, (rows, rows), 0)
        same = (near ^ lax.broadcasted_iota(jnp.int32, (rows, rows), 1)) < block
        s = jnp.where(key_pos < limit, dot_nt(keys, q) * score_scale, MASKED)
        s_own = jnp.where(same, dot_nt(own_keys, q[rows:]) * score_scale, MASKED)
        peak = jnp.max(s, axis=0, keepdims=True)
        peak_own = jnp.maximum(peak[:, rows:], jnp.max(s_own, axis=0, keepdims=True))
        peak = jnp.concatenate([peak[:, :rows], peak_own], axis=1)
        e = jnp.exp(s - peak)
        e_own = jnp.exp(s_own - peak_own)
        total = jnp.sum(e, axis=0, keepdims=True)
        total_own = total[:, rows:] + jnp.sum(e_own, axis=0, keepdims=True)
        inverse = 1.0 / jnp.concatenate([total[:, :rows], total_own], axis=1)
        p = e * inverse
        p_own = e_own * inverse[:, rows:]
        p_half = p.astype(jnp.bfloat16)
        p_half_own = p_own.astype(jnp.bfloat16)
        gp = dot_nt(values, g)
        gp_own = dot_nt(own_values, g[rows:])
        delta = jnp.sum(p_half.astype(jnp.float32) * gp, axis=0, keepdims=True)
        delta_own = delta[:, rows:] + jnp.sum(
            p_half_own.astype(jnp.float32) * gp_own, axis=0, keepdims=True
        )
        delta = jnp.concatenate([delta[:, :rows], delta_own], axis=1)
        ds = (p * (gp - delta)).astype(jnp.bfloat16)
        ds_own = (p_own * (gp_own - delta_own)).astype(jnp.bfloat16)
        dkv[:, :HEAD_DIM] += dot(ds, q)
        dkv[:, HEAD_DIM:] += dot(p_half, g)
        dn[:, :HEAD_DIM] += dot(ds_own, q[rows:])
        dn[:, HEAD_DIM:] += dot(p_half_own, g[rows:])
        dq = dot(kt[...], ds)
        dq_own = dq[:, rows:] + dot(knt[...], ds_own)
        dq_ref[:rows, columns] = (dq[:, :rows] * score_scale).T.astype(jnp.bfloat16)
        dq_ref[rows:, columns] = (dq_own * score_scale).T.astype(jnp.bfloat16)
        return carry

    lax.fori_loop(0, q_ref.shape[1] // HEAD_DIM, head_turn, 0)

    pair_scale = jnp.where(
        lax.broadcasted_iota(jnp.int32, (1, 2 * HEAD_DIM), 1) < HEAD_DIM, score_scale, 1.0
    )
    for block_at in range(n):
        pgp[block_at] = (dkv[block_at * rows : (block_at + 1) * rows] * pair_scale).astype(jnp.bfloat16)
    clean, noisy = pl.ds(0, rows), pl.ds(rows, rows)
    for off, peer in ctx_peers:
        put(pgp.at[peer], pin.at[me], pp_s.at[off], pp_r.at[me], context=peer)
    pga[me, noisy] = (dn[...] * pair_scale).astype(jnp.bfloat16)
    part = pga.at[me, noisy]
    put(part, pgo.at[noisy], po_sem.at[0], po_sem.at[1], head=other)
    for off, peer in ctx_peers:
        put(part, part, pn_s.at[off], pn_r.at[me], context=peer)
    clean_sum = dkv[my_rows, :] * pair_scale
    for off, src in ctx_peers:
        arrived(pin.at[src], pp_s.at[off], pp_r.at[src])
        clean_sum += pin[src].astype(jnp.float32)
    pga[me, clean] = clean_sum.astype(jnp.bfloat16)
    part = pga.at[me, clean]
    for off, peer in ctx_peers:
        put(part, part, pc_s.at[off], pc_r.at[me], context=peer)
    put(part, pgo.at[clean], po_sem.at[2], po_sem.at[3], head=other)

    for off, src in ctx_peers:
        for piece in range(2):
            span = token_rows(head, piece)
            part = tokd.at[src, span]
            arrived(part, td_s.at[piece, off], td_r.at[piece, src])
            put(part, part, tf_s.at[piece, off], tf_r.at[piece, src], head=other)
    own_tokens.wait()
    arrived(wo, wo_sem.at[0], wo_sem.at[1])
    arrived(pgo.at[noisy], po_sem.at[0], po_sem.at[1])
    arrived(pgo.at[clean], po_sem.at[2], po_sem.at[3])

    for at in range(half):
        gx_ref[:, at * wrows : (at + 1) * wrows] = (
            dot_nt(pga[me], wf[head * half + at]) + dot_nt(pgo[...], wo[at])
        ).astype(jnp.bfloat16)

    gw = dot(pga[me].T, tokd[me])
    for off, src in ctx_peers:
        for piece in range(2):
            span = token_rows(other, piece)
            arrived(tokd.at[src, span], tf_s.at[piece, off], tf_r.at[piece, src])
        arrived(pga.at[src, noisy], pn_s.at[off], pn_r.at[src])
        arrived(pga.at[src, clean], pc_s.at[off], pc_r.at[src])
        gw += dot(pga[src].T, tokd[src])

    slab = gw.shape[0] // m
    for at in range(m):
        gsum[at] = gw[at * slab : (at + 1) * slab]
        rp[at] = gw[at * slab : (at + 1) * slab].astype(jnp.bfloat16)
    for off, peer in dp_peers:
        put(rp.at[peer], rin.at[me_dp], rs_s.at[off], rs_r.at[me_dp], dp=peer)
    slab_sum = gsum[me_dp]
    for off, src in dp_peers:
        arrived(rin.at[src], rs_s.at[off], rs_r.at[src])
        slab_sum += rin[src].astype(jnp.float32)
    rall[me_dp] = slab_sum.astype(jnp.bfloat16)
    for off, peer in dp_peers:
        put(rall.at[me_dp], rall.at[me_dp], ra_s.at[off], ra_r.at[me_dp], dp=peer)
    for off, src in dp_peers:
        arrived(rall.at[src], ra_s.at[off], ra_r.at[src])
    for at in range(m):
        gw_ref[at * slab : (at + 1) * slab] = rall[at].astype(jnp.float32)
    for copy in sends:
        copy.wait_send()


def per_device(tokens, queries, grad_out, w_key, w_value, block_len):
    n = lax.axis_size("context")
    m = lax.axis_size("dp")
    rows = tokens.shape[2]
    features = tokens.shape[3]
    wrows, width = w_key.shape
    q_width = queries.shape[3]
    share = wrows * 7 // 8 // m // 16 * 16
    early = rows // 2
    half = n // 2
    pair = 2 * width
    bf16, f32 = jnp.bfloat16, jnp.float32
    vmem = pl.BlockSpec(memory_space=pltpu.VMEM)
    dma = pltpu.SemaphoreType.DMA
    slab = pair // m
    dq, gx, gw = pl.pallas_call(
        functools.partial(fused_kernel, n, m, share, early),
        out_shape=(
            jax.ShapeDtypeStruct((2 * rows, q_width), bf16),
            jax.ShapeDtypeStruct((2 * rows, features), bf16),
            jax.ShapeDtypeStruct((pair, wrows), f32),
        ),
        in_specs=[pl.BlockSpec(memory_space=pltpu.SMEM)] + [vmem] * 5,
        out_specs=(vmem, vmem, vmem),
        scratch_shapes=[
            pltpu.VMEM((2, 2 * rows, features), bf16),
            pltpu.VMEM((n, wrows, pair), bf16),
            pltpu.VMEM((half, wrows, pair), bf16),
            pltpu.VMEM((n * rows, pair), bf16),
            pltpu.VMEM((rows, pair), bf16),
            pltpu.VMEM((width, n * rows), bf16),
            pltpu.VMEM((width, rows), bf16),
            pltpu.VMEM((n * rows, pair), f32),
            pltpu.VMEM((rows, pair), f32),
            pltpu.VMEM((n, rows, pair), bf16),
            pltpu.VMEM((n, rows, pair), bf16),
            pltpu.VMEM((n, 2 * rows, pair), bf16),
            pltpu.VMEM((2 * rows, pair), bf16),
            pltpu.VMEM((n, 2 * rows, wrows), bf16),
            pltpu.VMEM((m, slab, wrows), f32),
            pltpu.VMEM((m, slab, wrows), bf16),
            pltpu.VMEM((m, slab, wrows), bf16),
            pltpu.VMEM((m, slab, wrows), bf16),
            dma((4,)), dma((2,)), dma((n,)), dma((n,)), dma((n,)), dma((n,)),
            dma((n, m)), dma((n, m)), dma((2,)), dma((n,)), dma((n,)),
            dma((2, n)), dma((2, n)), dma((2, n)), dma((2, n)),
            dma((n,)), dma((n,)), dma((n,)), dma((n,)), dma((n,)), dma((n,)),
            dma((4,)), dma((m,)), dma((m,)), dma((m,)), dma((m,)),
        ],
        compiler_params=pltpu.CompilerParams(
            collective_id=0, has_side_effects=True, vmem_limit_bytes=60 * 1024 * 1024
        ),
    )(
        block_len,
        tokens.reshape(2 * rows, features),
        queries.reshape(2 * rows, q_width),
        grad_out.reshape(2 * rows, q_width),
        w_key,
        w_value,
    )
    return (
        dq.reshape(queries.shape),
        gx.reshape(tokens.shape),
        gw[:width].T,
        gw[width:].T,
    )


def solution(mesh):
    placed = (
        P("dp", None, "context", "head"),
        P("dp", None, "context", "head"),
        P("dp", None, "context", "head"),
        P("context", "head"),
        P("context", "head"),
        P("dp"),
    )
    return jax.shard_map(
        per_device,
        mesh=mesh,
        in_specs=placed,
        out_specs=(
            P("dp", None, "context", "head"),
            P("dp", None, "context", "head"),
            P("context", "head"),
            P("context", "head"),
        ),
        check_vma=False,
    )
```

```python
import functools
import math

import jax
import jax.numpy as jnp
from jax import lax
from jax.experimental import pallas as pl
from jax.experimental.pallas import tpu as pltpu
from jax.sharding import PartitionSpec as P

HEAD_DIM = 128
MASKED = -1e30
MESH = pl.DeviceIdType.MESH
NT = (((1,), (1,)), ((), ()))


def near_first(count):
    order = []
    for step in range(1, count):
        for offset in (step, count - step):
            if offset not in order:
                order.append(offset)
    return order


def dot(left, right):
    return jnp.dot(left, right, preferred_element_type=jnp.float32)


def dot_nt(left, right):
    return lax.dot_general(left, right, NT, preferred_element_type=jnp.float32)


def fused_kernel(
    n, m, share, early,
    blk_ref, tok_ref, q_ref, g_ref, wk_ref, wv_ref,
    dq_ref, gx_ref, gwk_ref, gwv_ref,
    tokf, wf, wo, kv, kvn, kt, knt, dkv, dn, pgp, pin, pga, pgo, tokd, gsum, rp, rin, rall,
    loc_sem, tok_sem, wz_s, wz_r, wd_s, wd_r, wx_s, wx_r, wo_sem, kv_s, kv_r,
    td_s, td_r, tf_s, tf_r, pp_s, pp_r, pn_s, pn_r, pc_s, pc_r, po_sem, rs_s, rs_r, ra_s, ra_r,
):
    me_dp = lax.axis_index("dp")
    me = lax.axis_index("context")
    head = lax.axis_index("head")
    other = 1 - head
    rows2, features = tok_ref.shape
    rows = rows2 // 2
    wrows = wk_ref.shape[0]
    half = n // 2
    score_scale = 1.0 / math.sqrt(HEAD_DIM)
    sends = []

    def copy_of(src, dst, send_sem, recv_sem, **device):
        return pltpu.make_async_remote_copy(
            src_ref=src, dst_ref=dst, send_sem=send_sem, recv_sem=recv_sem,
            device_id=device, device_id_type=MESH,
        )

    def put(src, dst, send_sem, recv_sem, **device):
        copy = copy_of(src, dst, send_sem, recv_sem, **device)
        copy.start()
        sends.append((None, copy))

    def put_if(condition, src, dst, send_sem, recv_sem, **device):
        copy = copy_of(src, dst, send_sem, recv_sem, **device)
        pl.when(condition)(copy.start)
        sends.append((condition, copy))

    def arrived(dst, send_sem, recv_sem):
        copy_of(dst, dst, send_sem, recv_sem, head=other).wait_recv()

    ctx_peers = [(off, lax.rem(me + off, n)) for off in near_first(n)]
    dp_peers = [(off, lax.rem(me_dp + off, m)) for off in near_first(m)]

    two_step = m == 4 and share % 32 == 0
    if two_step:
        low = lax.rem(me_dp, 2)
        w_peers = [(0, me_dp + 1 - 2 * low), (1, lax.rem(me_dp + 2, 4))]
    else:
        w_peers = [(at, peer) for at, (_, peer) in enumerate(dp_peers)]

    own_copies = [
        pltpu.make_async_copy(wk_ref, wf.at[me, :, pl.ds(0, HEAD_DIM)], loc_sem.at[0]),
        pltpu.make_async_copy(wv_ref, wf.at[me, :, pl.ds(HEAD_DIM, HEAD_DIM)], loc_sem.at[1]),
        pltpu.make_async_copy(tok_ref, tokf.at[head], loc_sem.at[2]),
    ]
    for copy in own_copies:
        copy.start()

    barrier = pltpu.get_barrier_semaphore()
    for _, peer in ctx_peers:
        pl.semaphore_signal(barrier, inc=1, device_id={"context": peer}, device_id_type=MESH)
    for _, peer in dp_peers:
        pl.semaphore_signal(barrier, inc=1, device_id={"dp": peer}, device_id_type=MESH)
    pl.semaphore_signal(barrier, inc=1, device_id={"head": other}, device_id_type=MESH)
    pl.semaphore_wait(barrier, n + m - 1)

    put(tok_ref, tokf.at[head], tok_sem.at[0], tok_sem.at[1], head=other)
    own_copies[0].wait()
    own_copies[1].wait()
    shared = pl.ds(pl.multiple_of(me_dp * share, 16), share)
    direct_rows = wrows - m * share
    direct = pl.ds(m * share, direct_rows)
    for off, peer in ctx_peers:
        part = wf.at[me, shared]
        put(part, part, wz_s.at[off], wz_r.at[me], context=peer)
    if direct_rows:
        for off, peer in ctx_peers:
            part = wf.at[me, direct]
            put(part, part, wd_s.at[off], wd_r.at[me], context=peer)
    own_copies[2].wait()
    arrived(tokf.at[other], tok_sem.at[0], tok_sem.at[1])

    def token_block(owner):
        column = pl.multiple_of(lax.rem(owner, half) * wrows, 128)
        return owner // half, pl.ds(column, wrows)

    def token_rows(core, part):
        start = 0 if part == 0 else early
        count = early if part == 0 else rows - early
        return pl.ds(pl.multiple_of(core * rows + start, 16), count)

    def token_copy(part, off, peer):
        span = token_rows(head, part)
        side, columns = token_block(peer)
        return copy_of(
            tokf.at[side, span, columns], tokd.at[me, span],
            td_s.at[part, off], td_r.at[part, me], context=peer,
        )

    my_side, my_columns = token_block(me)
    own_tokens = pltpu.make_async_copy(tokf.at[my_side, :, my_columns], tokd.at[me], loc_sem.at[3])
    own_tokens.start()
    for off, src in ctx_peers:
        part = wf.at[src, shared]
        arrived(part, wz_s.at[off], wz_r.at[src])
        for dp_at, peer in w_peers:
            put(part, part, wx_s.at[src, dp_at], wx_r.at[src, dp_at], dp=peer)
    if two_step:
        for off, src in ctx_peers:
            for dp_at, peer in w_peers:
                base = pl.multiple_of(peer * share, 16)
                whole = wf.at[src, pl.ds(base, share)]
                arrived(whole, wx_s.at[src, dp_at], wx_r.at[src, dp_at])
                to = w_peers[1 - dp_at][1]
                start = 0 if dp_at == 0 else share // 2
                piece = wf.at[src, pl.ds(pl.multiple_of(base + start, 16), share // 2)]
                put(piece, piece, wx_s.at[src, 2 + dp_at], wx_r.at[src, 2 + dp_at], dp=to)
    for off, peer in ctx_peers:
        copy = token_copy(0, off, peer)
        copy.start()
        sends.append((None, copy))
    for off, peer in ctx_peers:
        copy = token_copy(1, off, peer)
        pl.when(peer < me)(copy.start)
        sends.append((None, copy))

    projected = dot(tokf[my_side, :, my_columns], wf[me])
    for off, src in ctx_peers:
        if direct_rows:
            arrived(wf.at[src, direct], wd_s.at[off], wd_r.at[src])
        if two_step:
            base = (3 - me_dp) * share
            for dp_at in range(2):
                start = 0 if dp_at == 0 else share // 2
                theirs = pl.ds(pl.multiple_of(base + start, 16), share // 2)
                arrived(wf.at[src, theirs], wx_s.at[src, 2 + dp_at], wx_r.at[src, 2 + dp_at])
        else:
            for dp_at, peer in w_peers:
                origin = lax.rem(me_dp + m - dp_peers[dp_at][0], m)
                theirs = pl.ds(pl.multiple_of(origin * share, 16), share)
                arrived(wf.at[src, theirs], wx_s.at[src, dp_at], wx_r.at[src, dp_at])
        side, columns = token_block(src)
        projected += dot(tokf[side, :, columns], wf[src])
    pairs = projected.astype(jnp.bfloat16)
    my_rows = pl.ds(pl.multiple_of(me * rows, rows), rows)
    kv[my_rows, :] = pairs[:rows]
    kvn[...] = pairs[rows:]
    for off, peer in ctx_peers:
        put_if(peer > me, kv.at[my_rows], kv.at[my_rows], kv_s.at[off], kv_r.at[me], context=peer)
    put(wf.at[pl.ds(other * half, half)], wo, wo_sem.at[0], wo_sem.at[1], head=other)
    for off, peer in ctx_peers:
        pl.when(peer > me)(token_copy(1, off, peer).start)

    block = blk_ref[0]
    total_rows = n * rows
    lane = lax.broadcasted_iota(jnp.int32, (1, rows2), 1)
    noisy_lane = lane >= rows
    position = me * rows + jnp.where(noisy_lane, lane - rows, lane)
    block_start = position & (-block)
    limit = jnp.where(noisy_lane, block_start, block_start + block)
    dkv[...] = jnp.zeros_like(dkv)
    dn[...] = jnp.zeros_like(dn)
    knt[...] = kvn[:, :HEAD_DIM].T
    for off, src in ctx_peers:
        span = pl.ds(pl.multiple_of(src * rows, rows), rows)

        @pl.when(src < me)
        def _(span=span, off=off, src=src):
            arrived(kv.at[span], kv_s.at[off], kv_r.at[src])

        @pl.when(src > me)
        def _(span=span):
            kv[span, :] = jnp.zeros((rows, 2 * HEAD_DIM), jnp.bfloat16)
    kt[...] = kv[:, :HEAD_DIM].T

    def head_turn(turn, carry):
        columns = pl.ds(pl.multiple_of(turn * HEAD_DIM, HEAD_DIM), HEAD_DIM)
        q = q_ref[:, columns]
        g = g_ref[:, columns]
        keys = kv[:, :HEAD_DIM]
        values = kv[:, HEAD_DIM:]
        own_keys = kvn[:, :HEAD_DIM]
        own_values = kvn[:, HEAD_DIM:]
        key_pos = lax.broadcasted_iota(jnp.int32, (total_rows, rows2), 0)
        near = lax.broadcasted_iota(jnp.int32, (rows, rows), 0)
        same = (near ^ lax.broadcasted_iota(jnp.int32, (rows, rows), 1)) < block
        s = jnp.where(key_pos < limit, dot_nt(keys, q) * score_scale, MASKED)
        s_own = jnp.where(same, dot_nt(own_keys, q[rows:]) * score_scale, MASKED)
        peak = jnp.max(s, axis=0, keepdims=True)
        peak_own = jnp.maximum(peak[:, rows:], jnp.max(s_own, axis=0, keepdims=True))
        peak = jnp.concatenate([peak[:, :rows], peak_own], axis=1)
        e = jnp.exp(s - peak)
        e_own = jnp.exp(s_own - peak_own)
        total = jnp.sum(e, axis=0, keepdims=True)
        total_own = total[:, rows:] + jnp.sum(e_own, axis=0, keepdims=True)
        inverse = 1.0 / jnp.concatenate([total[:, :rows], total_own], axis=1)
        p = e * inverse
        p_own = e_own * inverse[:, rows:]
        p_half = p.astype(jnp.bfloat16)
        p_half_own = p_own.astype(jnp.bfloat16)
        gp = dot_nt(values, g)
        gp_own = dot_nt(own_values, g[rows:])
        delta = jnp.sum(p_half.astype(jnp.float32) * gp, axis=0, keepdims=True)
        delta_own = delta[:, rows:] + jnp.sum(
            p_half_own.astype(jnp.float32) * gp_own, axis=0, keepdims=True
        )
        delta = jnp.concatenate([delta[:, :rows], delta_own], axis=1)
        ds = (p * (gp - delta)).astype(jnp.bfloat16)
        ds_own = (p_own * (gp_own - delta_own)).astype(jnp.bfloat16)
        dkv[:, :HEAD_DIM] += dot(ds, q)
        dkv[:, HEAD_DIM:] += dot(p_half, g)
        dn[:, :HEAD_DIM] += dot(ds_own, q[rows:])
        dn[:, HEAD_DIM:] += dot(p_half_own, g[rows:])
        dq = dot(kt[...], ds)
        dq_own = dq[:, rows:] + dot(knt[...], ds_own)
        dq_ref[:rows, columns] = (dq[:, :rows] * score_scale).T.astype(jnp.bfloat16)
        dq_ref[rows:, columns] = (dq_own * score_scale).T.astype(jnp.bfloat16)
        return carry

    lax.fori_loop(0, q_ref.shape[1] // HEAD_DIM, head_turn, 0)

    pair_scale = jnp.where(
        lax.broadcasted_iota(jnp.int32, (1, 2 * HEAD_DIM), 1) < HEAD_DIM, score_scale, 1.0
    )
    for block_at in range(n):
        pgp[block_at] = (dkv[block_at * rows : (block_at + 1) * rows] * pair_scale).astype(jnp.bfloat16)
    clean, noisy = pl.ds(0, rows), pl.ds(rows, rows)
    for off, peer in ctx_peers:
        put_if(peer < me, pgp.at[peer], pin.at[me], pp_s.at[off], pp_r.at[me], context=peer)
    pga[me, noisy] = (dn[...] * pair_scale).astype(jnp.bfloat16)
    part = pga.at[me, noisy]
    put(part, pgo.at[noisy], po_sem.at[0], po_sem.at[1], head=other)
    for off, peer in ctx_peers:
        put(part, part, pn_s.at[off], pn_r.at[me], context=peer)
    dkv[my_rows, :] *= pair_scale
    for off, src in ctx_peers:

        @pl.when(src > me)
        def _(off=off, src=src):
            arrived(pin.at[src], pp_s.at[off], pp_r.at[src])
            dkv[my_rows, :] += pin[src].astype(jnp.float32)

    pga[me, clean] = dkv[my_rows, :].astype(jnp.bfloat16)
    part = pga.at[me, clean]
    for off, peer in ctx_peers:
        put(part, part, pc_s.at[off], pc_r.at[me], context=peer)
    put(part, pgo.at[clean], po_sem.at[2], po_sem.at[3], head=other)

    for off, src in ctx_peers:
        for piece in range(2):
            span = token_rows(head, piece)
            part = tokd.at[src, span]
            arrived(part, td_s.at[piece, off], td_r.at[piece, src])
            put(part, part, tf_s.at[piece, off], tf_r.at[piece, src], head=other)
    own_tokens.wait()
    arrived(wo, wo_sem.at[0], wo_sem.at[1])
    arrived(pgo.at[noisy], po_sem.at[0], po_sem.at[1])
    arrived(pgo.at[clean], po_sem.at[2], po_sem.at[3])

    for at in range(half):
        gx_ref[:, at * wrows : (at + 1) * wrows] = (
            dot_nt(pga[me], wf[head * half + at]) + dot_nt(pgo[...], wo[at])
        ).astype(jnp.bfloat16)

    gw = dot(pga[me].T, tokd[me])
    for off, src in ctx_peers:
        for piece in range(2):
            span = token_rows(other, piece)
            arrived(tokd.at[src, span], tf_s.at[piece, off], tf_r.at[piece, src])
        arrived(pga.at[src, noisy], pn_s.at[off], pn_r.at[src])
        arrived(pga.at[src, clean], pc_s.at[off], pc_r.at[src])
        gw += dot(pga[src].T, tokd[src])

    slab = gw.shape[0] // m
    for at in range(m):
        gsum[at] = gw[at * slab : (at + 1) * slab]
        rp[at] = gw[at * slab : (at + 1) * slab].astype(jnp.bfloat16)
    for off, peer in dp_peers:
        put(rp.at[peer], rin.at[me_dp], rs_s.at[off], rs_r.at[me_dp], dp=peer)
    slab_sum = gsum[me_dp]
    for off, src in dp_peers:
        arrived(rin.at[src], rs_s.at[off], rs_r.at[src])
        slab_sum += rin[src].astype(jnp.float32)
    rall[me_dp] = slab_sum.astype(jnp.bfloat16)
    for off, peer in dp_peers:
        put(rall.at[me_dp], rall.at[me_dp], ra_s.at[off], ra_r.at[me_dp], dp=peer)
    for off, src in dp_peers:
        arrived(rall.at[src], ra_s.at[off], ra_r.at[src])
    for at in range(m):
        gsum[at] = rall[at].astype(jnp.float32)
    gwk_ref[...] = gsum[: m // 2].reshape(HEAD_DIM, wrows).T
    gwv_ref[...] = gsum[m // 2 :].reshape(HEAD_DIM, wrows).T
    for condition, copy in sends:
        if condition is None:
            copy.wait_send()
        else:
            pl.when(condition)(copy.wait_send)


def per_device(tokens, queries, grad_out, w_key, w_value, block_len):
    n = lax.axis_size("context")
    m = lax.axis_size("dp")
    rows = tokens.shape[2]
    features = tokens.shape[3]
    wrows, width = w_key.shape
    q_width = queries.shape[3]
    share = wrows // m // 16 * 16
    early = min(16, rows // 2)
    half = n // 2
    pair = 2 * width
    bf16, f32 = jnp.bfloat16, jnp.float32
    vmem = pl.BlockSpec(memory_space=pltpu.VMEM)
    dma = pltpu.SemaphoreType.DMA
    slab = pair // m
    dq, gx, gwk, gwv = pl.pallas_call(
        functools.partial(fused_kernel, n, m, share, early),
        out_shape=(
            jax.ShapeDtypeStruct((2 * rows, q_width), bf16),
            jax.ShapeDtypeStruct((2 * rows, features), bf16),
            jax.ShapeDtypeStruct((wrows, width), f32),
            jax.ShapeDtypeStruct((wrows, width), f32),
        ),
        in_specs=[pl.BlockSpec(memory_space=pltpu.SMEM)] + [vmem] * 5,
        out_specs=(vmem, vmem, vmem, vmem),
        scratch_shapes=[
            pltpu.VMEM((2, 2 * rows, features), bf16),
            pltpu.VMEM((n, wrows, pair), bf16),
            pltpu.VMEM((half, wrows, pair), bf16),
            pltpu.VMEM((n * rows, pair), bf16),
            pltpu.VMEM((rows, pair), bf16),
            pltpu.VMEM((width, n * rows), bf16),
            pltpu.VMEM((width, rows), bf16),
            pltpu.VMEM((n * rows, pair), f32),
            pltpu.VMEM((rows, pair), f32),
            pltpu.VMEM((n, rows, pair), bf16),
            pltpu.VMEM((n, rows, pair), bf16),
            pltpu.VMEM((n, 2 * rows, pair), bf16),
            pltpu.VMEM((2 * rows, pair), bf16),
            pltpu.VMEM((n, 2 * rows, wrows), bf16),
            pltpu.VMEM((m, slab, wrows), f32),
            pltpu.VMEM((m, slab, wrows), bf16),
            pltpu.VMEM((m, slab, wrows), bf16),
            pltpu.VMEM((m, slab, wrows), bf16),
            dma((4,)), dma((2,)), dma((n,)), dma((n,)), dma((n,)), dma((n,)),
            dma((n, m)), dma((n, m)), dma((2,)), dma((n,)), dma((n,)),
            dma((2, n)), dma((2, n)), dma((2, n)), dma((2, n)),
            dma((n,)), dma((n,)), dma((n,)), dma((n,)), dma((n,)), dma((n,)),
            dma((4,)), dma((m,)), dma((m,)), dma((m,)), dma((m,)),
        ],
        compiler_params=pltpu.CompilerParams(
            collective_id=0, has_side_effects=True, vmem_limit_bytes=60 * 1024 * 1024
        ),
    )(
        block_len,
        tokens.reshape(2 * rows, features),
        queries.reshape(2 * rows, q_width),
        grad_out.reshape(2 * rows, q_width),
        w_key,
        w_value,
    )
    return (
        dq.reshape(queries.shape),
        gx.reshape(tokens.shape),
        gwk,
        gwv,
    )


def solution(mesh):
    placed = (
        P("dp", None, "context", "head"),
        P("dp", None, "context", "head"),
        P("dp", None, "context", "head"),
        P("context", "head"),
        P("context", "head"),
        P("dp"),
    )
    return jax.shard_map(
        per_device,
        mesh=mesh,
        in_specs=placed,
        out_specs=(
            P("dp", None, "context", "head"),
            P("dp", None, "context", "head"),
            P("context", "head"),
            P("context", "head"),
        ),
        check_vma=False,
    )
```

```python
import functools
import math

import jax
import jax.numpy as jnp
from jax import lax
from jax.experimental import pallas as pl
from jax.experimental.pallas import tpu as pltpu
from jax.sharding import PartitionSpec as P

HEAD_DIM = 128
MASKED = -1e30
MESH = pl.DeviceIdType.MESH
NT = (((1,), (1,)), ((), ()))


def near_first(count):
    order = []
    for step in range(1, count):
        for offset in (step, count - step):
            if offset not in order:
                order.append(offset)
    return order


def dot(left, right):
    return jnp.dot(left, right, preferred_element_type=jnp.float32)


def dot_nt(left, right):
    return lax.dot_general(left, right, NT, preferred_element_type=jnp.float32)


def fused_kernel(
    n, m, share, early,
    blk_ref, tok_ref, q_ref, g_ref, wk_ref, wv_ref,
    dq_ref, gx_ref, gwk_ref, gwv_ref,
    tokf, wf, wo, kv, kvn, kt, knt, dkv, dn, pgp, pin, pga, pgo, tokd, gsum, rp, rin, rall,
    loc_sem, tok_sem, wz_s, wz_r, wd_s, wd_r, wx_s, wx_r, wo_sem, kv_s, kv_r,
    td_s, td_r, tf_s, tf_r, pp_s, pp_r, pn_s, pn_r, pc_s, pc_r, po_sem, rs_s, rs_r, ra_s, ra_r,
):
    me_dp = lax.axis_index("dp")
    me = lax.axis_index("context")
    head = lax.axis_index("head")
    other = 1 - head
    rows2, features = tok_ref.shape
    rows = rows2 // 2
    wrows = wk_ref.shape[0]
    half = n // 2
    score_scale = 1.0 / math.sqrt(HEAD_DIM)
    sends = []

    def copy_of(src, dst, send_sem, recv_sem, **device):
        return pltpu.make_async_remote_copy(
            src_ref=src, dst_ref=dst, send_sem=send_sem, recv_sem=recv_sem,
            device_id=device, device_id_type=MESH,
        )

    def put(src, dst, send_sem, recv_sem, **device):
        copy = copy_of(src, dst, send_sem, recv_sem, **device)
        copy.start()
        sends.append((None, copy))

    def put_if(condition, src, dst, send_sem, recv_sem, **device):
        copy = copy_of(src, dst, send_sem, recv_sem, **device)
        pl.when(condition)(copy.start)
        sends.append((condition, copy))

    def arrived(dst, send_sem, recv_sem):
        copy_of(dst, dst, send_sem, recv_sem, head=other).wait_recv()

    ctx_peers = [(off, lax.rem(me + off, n)) for off in near_first(n)]
    dp_peers = [(off, lax.rem(me_dp + off, m)) for off in near_first(m)]

    two_step = m == 4 and share % 32 == 0
    if two_step:
        low = lax.rem(me_dp, 2)
        w_peers = [(0, me_dp + 1 - 2 * low), (1, lax.rem(me_dp + 2, 4))]
    else:
        w_peers = [(at, peer) for at, (_, peer) in enumerate(dp_peers)]

    own_copies = [
        pltpu.make_async_copy(wk_ref, wf.at[me, :, pl.ds(0, HEAD_DIM)], loc_sem.at[0]),
        pltpu.make_async_copy(wv_ref, wf.at[me, :, pl.ds(HEAD_DIM, HEAD_DIM)], loc_sem.at[1]),
        pltpu.make_async_copy(tok_ref, tokf.at[head], loc_sem.at[2]),
    ]
    for copy in own_copies:
        copy.start()

    barrier = pltpu.get_barrier_semaphore()
    for _, peer in ctx_peers:
        pl.semaphore_signal(barrier, inc=1, device_id={"context": peer}, device_id_type=MESH)
    for _, peer in dp_peers:
        pl.semaphore_signal(barrier, inc=1, device_id={"dp": peer}, device_id_type=MESH)
    pl.semaphore_signal(barrier, inc=1, device_id={"head": other}, device_id_type=MESH)
    pl.semaphore_wait(barrier, n + m - 1)

    put(tok_ref, tokf.at[head], tok_sem.at[0], tok_sem.at[1], head=other)
    own_copies[0].wait()
    own_copies[1].wait()
    shared = pl.ds(pl.multiple_of(me_dp * share, 16), share)
    direct_rows = wrows - m * share
    direct = pl.ds(m * share, direct_rows)
    for off, peer in ctx_peers:
        part = wf.at[me, shared]
        put(part, part, wz_s.at[off], wz_r.at[me], context=peer)
    if direct_rows:
        for off, peer in ctx_peers:
            part = wf.at[me, direct]
            put(part, part, wd_s.at[off], wd_r.at[me], context=peer)
    own_copies[2].wait()
    arrived(tokf.at[other], tok_sem.at[0], tok_sem.at[1])

    def token_block(owner):
        column = pl.multiple_of(lax.rem(owner, half) * wrows, 128)
        return owner // half, pl.ds(column, wrows)

    def token_rows(core, part):
        start = 0 if part == 0 else early
        count = early if part == 0 else rows - early
        return pl.ds(pl.multiple_of(core * rows + start, 16), count)

    def token_copy(part, off, peer):
        span = token_rows(head, part)
        side, columns = token_block(peer)
        return copy_of(
            tokf.at[side, span, columns], tokd.at[me, span],
            td_s.at[part, off], td_r.at[part, me], context=peer,
        )

    my_side, my_columns = token_block(me)
    own_tokens = pltpu.make_async_copy(tokf.at[my_side, :, my_columns], tokd.at[me], loc_sem.at[3])
    own_tokens.start()
    for off, src in ctx_peers:
        part = wf.at[src, shared]
        arrived(part, wz_s.at[off], wz_r.at[src])
        for dp_at, peer in w_peers:
            put(part, part, wx_s.at[src, dp_at], wx_r.at[src, dp_at], dp=peer)
    if two_step:
        for off, src in ctx_peers:
            for dp_at, peer in w_peers:
                base = pl.multiple_of(peer * share, 16)
                whole = wf.at[src, pl.ds(base, share)]
                arrived(whole, wx_s.at[src, dp_at], wx_r.at[src, dp_at])
                to = w_peers[1 - dp_at][1]
                start = 0 if dp_at == 0 else share // 2
                piece = wf.at[src, pl.ds(pl.multiple_of(base + start, 16), share // 2)]
                put(piece, piece, wx_s.at[src, 2 + dp_at], wx_r.at[src, 2 + dp_at], dp=to)
    for off, peer in ctx_peers:
        copy = token_copy(0, off, peer)
        copy.start()
        sends.append((None, copy))
    for off, peer in ctx_peers:
        copy = token_copy(1, off, peer)
        pl.when(peer < me)(copy.start)
        sends.append((None, copy))

    projected = dot(tokf[my_side, :, my_columns], wf[me])
    for off, src in ctx_peers:
        if direct_rows:
            arrived(wf.at[src, direct], wd_s.at[off], wd_r.at[src])
        if two_step:
            base = (3 - me_dp) * share
            for dp_at in range(2):
                start = 0 if dp_at == 0 else share // 2
                theirs = pl.ds(pl.multiple_of(base + start, 16), share // 2)
                arrived(wf.at[src, theirs], wx_s.at[src, 2 + dp_at], wx_r.at[src, 2 + dp_at])
        else:
            for dp_at, peer in w_peers:
                origin = lax.rem(me_dp + m - dp_peers[dp_at][0], m)
                theirs = pl.ds(pl.multiple_of(origin * share, 16), share)
                arrived(wf.at[src, theirs], wx_s.at[src, dp_at], wx_r.at[src, dp_at])
        side, columns = token_block(src)
        projected += dot(tokf[side, :, columns], wf[src])
    pairs = projected.astype(jnp.bfloat16)
    my_rows = pl.ds(pl.multiple_of(me * rows, rows), rows)
    kv[my_rows, :] = pairs[:rows]
    kvn[...] = pairs[rows:]
    for off, peer in ctx_peers:
        put_if(peer > me, kv.at[my_rows], kv.at[my_rows], kv_s.at[off], kv_r.at[me], context=peer)
    put(wf.at[pl.ds(other * half, half)], wo, wo_sem.at[0], wo_sem.at[1], head=other)
    for off, peer in ctx_peers:
        pl.when(peer > me)(token_copy(1, off, peer).start)

    block = blk_ref[0]
    total_rows = n * rows
    lane = lax.broadcasted_iota(jnp.int32, (1, rows2), 1)
    noisy_lane = lane >= rows
    position = me * rows + jnp.where(noisy_lane, lane - rows, lane)
    block_start = position & (-block)
    limit = jnp.where(noisy_lane, block_start, block_start + block)
    dkv[...] = jnp.zeros_like(dkv)
    dn[...] = jnp.zeros_like(dn)
    knt[...] = kvn[:, :HEAD_DIM].T
    for off, src in ctx_peers:
        span = pl.ds(pl.multiple_of(src * rows, rows), rows)

        @pl.when(src < me)
        def _(span=span, off=off, src=src):
            arrived(kv.at[span], kv_s.at[off], kv_r.at[src])

        @pl.when(src > me)
        def _(span=span):
            kv[span, :] = jnp.zeros((rows, 2 * HEAD_DIM), jnp.bfloat16)
    kt[...] = kv[:, :HEAD_DIM].T

    def head_turn(turn, carry):
        columns = pl.ds(pl.multiple_of(turn * HEAD_DIM, HEAD_DIM), HEAD_DIM)
        q = q_ref[:, columns]
        g = g_ref[:, columns]
        keys = kv[:, :HEAD_DIM]
        values = kv[:, HEAD_DIM:]
        own_keys = kvn[:, :HEAD_DIM]
        own_values = kvn[:, HEAD_DIM:]
        key_pos = lax.broadcasted_iota(jnp.int32, (total_rows, rows2), 0)
        near = lax.broadcasted_iota(jnp.int32, (rows, rows), 0)
        same = (near ^ lax.broadcasted_iota(jnp.int32, (rows, rows), 1)) < block
        s = jnp.where(key_pos < limit, dot_nt(keys, q) * score_scale, MASKED)
        s_own = jnp.where(same, dot_nt(own_keys, q[rows:]) * score_scale, MASKED)
        peak = jnp.max(s, axis=0, keepdims=True)
        peak_own = jnp.maximum(peak[:, rows:], jnp.max(s_own, axis=0, keepdims=True))
        peak = jnp.concatenate([peak[:, :rows], peak_own], axis=1)
        e = jnp.exp(s - peak)
        e_own = jnp.exp(s_own - peak_own)
        total = jnp.sum(e, axis=0, keepdims=True)
        total_own = total[:, rows:] + jnp.sum(e_own, axis=0, keepdims=True)
        inverse = 1.0 / jnp.concatenate([total[:, :rows], total_own], axis=1)
        p = e * inverse
        p_own = e_own * inverse[:, rows:]
        p_half = p.astype(jnp.bfloat16)
        p_half_own = p_own.astype(jnp.bfloat16)
        gp = dot_nt(values, g)
        gp_own = dot_nt(own_values, g[rows:])
        delta = jnp.sum(p_half.astype(jnp.float32) * gp, axis=0, keepdims=True)
        delta_own = delta[:, rows:] + jnp.sum(
            p_half_own.astype(jnp.float32) * gp_own, axis=0, keepdims=True
        )
        delta = jnp.concatenate([delta[:, :rows], delta_own], axis=1)
        ds = (p * (gp - delta)).astype(jnp.bfloat16)
        ds_own = (p_own * (gp_own - delta_own)).astype(jnp.bfloat16)
        dkv[:, :HEAD_DIM] += dot(ds, q)
        dkv[:, HEAD_DIM:] += dot(p_half, g)
        dn[:, :HEAD_DIM] += dot(ds_own, q[rows:])
        dn[:, HEAD_DIM:] += dot(p_half_own, g[rows:])
        dq = dot(kt[...], ds)
        dq_own = dq[:, rows:] + dot(knt[...], ds_own)
        dq_ref[:rows, columns] = (dq[:, :rows] * score_scale).T.astype(jnp.bfloat16)
        dq_ref[rows:, columns] = (dq_own * score_scale).T.astype(jnp.bfloat16)
        return carry

    lax.fori_loop(0, q_ref.shape[1] // HEAD_DIM, head_turn, 0)

    pair_scale = jnp.where(
        lax.broadcasted_iota(jnp.int32, (1, 2 * HEAD_DIM), 1) < HEAD_DIM, score_scale, 1.0
    )
    for block_at in range(n):
        pgp[block_at] = (dkv[block_at * rows : (block_at + 1) * rows] * pair_scale).astype(jnp.bfloat16)
    clean, noisy = pl.ds(0, rows), pl.ds(rows, rows)
    for off, peer in ctx_peers:
        put_if(peer < me, pgp.at[peer], pin.at[me], pp_s.at[off], pp_r.at[me], context=peer)
    pga[me, noisy] = (dn[...] * pair_scale).astype(jnp.bfloat16)
    part = pga.at[me, noisy]
    put(part, pgo.at[noisy], po_sem.at[0], po_sem.at[1], head=other)
    for off, peer in ctx_peers:
        put(part, part, pn_s.at[off], pn_r.at[me], context=peer)
    dkv[my_rows, :] *= pair_scale
    for off, src in ctx_peers:

        @pl.when(src > me)
        def _(off=off, src=src):
            arrived(pin.at[src], pp_s.at[off], pp_r.at[src])
            dkv[my_rows, :] += pin[src].astype(jnp.float32)

    pga[me, clean] = dkv[my_rows, :].astype(jnp.bfloat16)
    part = pga.at[me, clean]
    for off, peer in ctx_peers:
        put(part, part, pc_s.at[off], pc_r.at[me], context=peer)
    put(part, pgo.at[clean], po_sem.at[2], po_sem.at[3], head=other)

    for off, src in ctx_peers:
        for piece in range(2):
            span = token_rows(head, piece)
            part = tokd.at[src, span]
            arrived(part, td_s.at[piece, off], td_r.at[piece, src])
            put(part, part, tf_s.at[piece, off], tf_r.at[piece, src], head=other)
    own_tokens.wait()
    arrived(wo, wo_sem.at[0], wo_sem.at[1])
    arrived(pgo.at[noisy], po_sem.at[0], po_sem.at[1])
    arrived(pgo.at[clean], po_sem.at[2], po_sem.at[3])

    for at in range(half):
        gx_ref[:, at * wrows : (at + 1) * wrows] = (
            dot_nt(pga[me], wf[head * half + at]) + dot_nt(pgo[...], wo[at])
        ).astype(jnp.bfloat16)

    gw = dot(pga[me].T, tokd[me])
    for off, src in ctx_peers:
        for piece in range(2):
            span = token_rows(other, piece)
            arrived(tokd.at[src, span], tf_s.at[piece, off], tf_r.at[piece, src])
        arrived(pga.at[src, noisy], pn_s.at[off], pn_r.at[src])
        arrived(pga.at[src, clean], pc_s.at[off], pc_r.at[src])
        gw += dot(pga[src].T, tokd[src])

    slab = gw.shape[0] // m
    for at in range(m):
        gsum[at] = gw[at * slab : (at + 1) * slab]
        rp[at] = gw[at * slab : (at + 1) * slab].astype(jnp.bfloat16)
    for off, peer in dp_peers:
        put(rp.at[peer], rin.at[me_dp], rs_s.at[off], rs_r.at[me_dp], dp=peer)
    slab_sum = gsum[me_dp]
    for off, src in dp_peers:
        arrived(rin.at[src], rs_s.at[off], rs_r.at[src])
        slab_sum += rin[src].astype(jnp.float32)
    rall[me_dp] = slab_sum.astype(jnp.bfloat16)
    for off, peer in dp_peers:
        put(rall.at[me_dp], rall.at[me_dp], ra_s.at[off], ra_r.at[me_dp], dp=peer)
    for off, src in dp_peers:
        arrived(rall.at[src], ra_s.at[off], ra_r.at[src])
    for at in range(m):
        gsum[at] = rall[at].astype(jnp.float32)
    gwk_ref[...] = gsum[: m // 2].reshape(HEAD_DIM, wrows).T
    gwv_ref[...] = gsum[m // 2 :].reshape(HEAD_DIM, wrows).T
    for condition, copy in sends:
        if condition is None:
            copy.wait_send()
        else:
            pl.when(condition)(copy.wait_send)


def per_device(tokens, queries, grad_out, w_key, w_value, block_len):
    n = lax.axis_size("context")
    m = lax.axis_size("dp")
    rows = tokens.shape[2]
    features = tokens.shape[3]
    wrows, width = w_key.shape
    q_width = queries.shape[3]
    share = wrows // m // 16 * 16
    early = max(16, rows // 64 * 16)
    half = n // 2
    pair = 2 * width
    bf16, f32 = jnp.bfloat16, jnp.float32
    vmem = pl.BlockSpec(memory_space=pltpu.VMEM)
    dma = pltpu.SemaphoreType.DMA
    slab = pair // m
    dq, gx, gwk, gwv = pl.pallas_call(
        functools.partial(fused_kernel, n, m, share, early),
        out_shape=(
            jax.ShapeDtypeStruct((2 * rows, q_width), bf16),
            jax.ShapeDtypeStruct((2 * rows, features), bf16),
            jax.ShapeDtypeStruct((wrows, width), f32),
            jax.ShapeDtypeStruct((wrows, width), f32),
        ),
        in_specs=[pl.BlockSpec(memory_space=pltpu.SMEM)] + [vmem] * 5,
        out_specs=(vmem, vmem, vmem, vmem),
        scratch_shapes=[
            pltpu.VMEM((2, 2 * rows, features), bf16),
            pltpu.VMEM((n, wrows, pair), bf16),
            pltpu.VMEM((half, wrows, pair), bf16),
            pltpu.VMEM((n * rows, pair), bf16),
            pltpu.VMEM((rows, pair), bf16),
            pltpu.VMEM((width, n * rows), bf16),
            pltpu.VMEM((width, rows), bf16),
            pltpu.VMEM((n * rows, pair), f32),
            pltpu.VMEM((rows, pair), f32),
            pltpu.VMEM((n, rows, pair), bf16),
            pltpu.VMEM((n, rows, pair), bf16),
            pltpu.VMEM((n, 2 * rows, pair), bf16),
            pltpu.VMEM((2 * rows, pair), bf16),
            pltpu.VMEM((n, 2 * rows, wrows), bf16),
            pltpu.VMEM((m, slab, wrows), f32),
            pltpu.VMEM((m, slab, wrows), bf16),
            pltpu.VMEM((m, slab, wrows), bf16),
            pltpu.VMEM((m, slab, wrows), bf16),
            dma((4,)), dma((2,)), dma((n,)), dma((n,)), dma((n,)), dma((n,)),
            dma((n, m)), dma((n, m)), dma((2,)), dma((n,)), dma((n,)),
            dma((2, n)), dma((2, n)), dma((2, n)), dma((2, n)),
            dma((n,)), dma((n,)), dma((n,)), dma((n,)), dma((n,)), dma((n,)),
            dma((4,)), dma((m,)), dma((m,)), dma((m,)), dma((m,)),
        ],
        compiler_params=pltpu.CompilerParams(
            collective_id=0, has_side_effects=True, vmem_limit_bytes=60 * 1024 * 1024
        ),
    )(
        block_len,
        tokens.reshape(2 * rows, features),
        queries.reshape(2 * rows, q_width),
        grad_out.reshape(2 * rows, q_width),
        w_key,
        w_value,
    )
    return (
        dq.reshape(queries.shape),
        gx.reshape(tokens.shape),
        gwk,
        gwv,
    )


def solution(mesh):
    placed = (
        P("dp", None, "context", "head"),
        P("dp", None, "context", "head"),
        P("dp", None, "context", "head"),
        P("context", "head"),
        P("context", "head"),
        P("dp"),
    )
    return jax.shard_map(
        per_device,
        mesh=mesh,
        in_specs=placed,
        out_specs=(
            P("dp", None, "context", "head"),
            P("dp", None, "context", "head"),
            P("context", "head"),
            P("context", "head"),
        ),
        check_vma=False,
    )
```
